32 devices in a mesh: ctx: 8 (over z, x), tp: 4 (over y, core).
Axes of the slice: x: 2, y: 2, z: 4, core: 2. Of those that a mesh axis runs over, the one named last changes fastest.
Arguments:
- layer_input: bfloat16 [2, 2048, 2048], P(None, 'ctx')
- attn_gain: bfloat16 [2048], replicated, may hold values from 0.5 to 1.5
- w_query: bfloat16 [2048, 2048], P(None, 'tp'), may hold values from -0.125 to 0.125
- w_key: bfloat16 [2048, 512], P(None, 'tp'), may hold values from -0.125 to 0.125
- w_value: bfloat16 [2048, 512], P(None, 'tp'), may hold values from -0.125 to 0.125
- w_out: bfloat16 [2048, 2048], P('tp'), may hold values from -3 to 3
- ffn_gain: bfloat16 [2048], replicated, may hold values from 0.5 to 1.5
- w_gate: bfloat16 [2048, 8192], P(None, 'tp'), may hold values from -0.125 to 0.125
- w_up: bfloat16 [2048, 8192], P(None, 'tp'), may hold values from -0.125 to 0.125
- w_down: bfloat16 [8192, 2048], P('tp'), may hold values from -0.0625 to 0.0625
- cotangent: bfloat16 [2, 2048, 2048], P(None, 'ctx'), may hold values from -6 to 6
- block_ids: int32 [2, 16], replicated, may hold values from 0 to 15, as said below
- doc_ids: int32 [2, 2048], replicated, may hold values from 0 to 2, never falling along the last dimension, each value on 1 to 1024 neighbouring positions
Outputs:
- block_out: bfloat16 [2, 2048, 2048], P(None, 'ctx')
- grad_input: float32 [2, 2048, 2048], P(None, 'ctx')
- grad_attn_gain: float32 [2048], P('ctx')
- grad_w_query: float32 [2048, 2048], P('ctx', 'tp')
- grad_w_key: float32 [2048, 512], P('ctx', 'tp')
- grad_w_value: float32 [2048, 512], P('ctx', 'tp')
- grad_w_out: float32 [2048, 2048], P('tp', 'ctx')
- grad_ffn_gain: float32 [2048], P('ctx')
- grad_w_gate: float32 [2048, 8192], P('ctx', 'tp')
- grad_w_up: float32 [2048, 8192], P('ctx', 'tp')
- grad_w_down: float32 [8192, 2048], P('tp', 'ctx')
The draws below stay inside these ranges and needn't reach their ends.
Inputs may be any that keep to these rules, and one draw needn't show every extreme that they name: `block_ids`: in each sequence every block number appears once, and the two slots 2 c and 2 c + 1 hold blocks b and 15 - b. `doc_ids`: document numbers never fall along positions; a document spans at most 1024 positions, and one spans exactly that many.
All inputs are finite; a program needn't handle non-finite values.
Results may differ from the reference program's by a relative error of at most 0.013.
Values may be sent and summed in bfloat16 or wider, within the bound.
A program may use at most 1.0625 GiB of HBM per device.

```python
import math
import jax
import jax.numpy as jnp
import numpy as np
from jax import lax

D = 2048
HEADS = 32
KV_HEADS = 8
HEAD_DIM = 64
FF = 8192
BLK = 128
SEQS = 2
NBLK = 16
LENGTH = 2048


def draw_layer_input(key, part):
    key_base, key_rows, key_cols = jax.random.split(key, 3)
    base = jax.random.normal(key_base, (SEQS, LENGTH, D), jnp.float32)
    row_spread = math.log(2.0)
    col_spread = math.log(2.0)
    rows = jnp.exp(jax.random.uniform(key_rows, (SEQS, LENGTH, 1), jnp.float32) * row_spread)
    cols = jnp.exp(jax.random.uniform(key_cols, (1, 1, D), jnp.float32) * col_spread)
    return (base * rows * cols).astype(jnp.bfloat16)


def draw_block_ids(key, part):
    half_count = NBLK // 2
    key_perm, key_flip = jax.random.split(key, 2)
    perm_keys = jax.random.split(key_perm, SEQS)
    pairs = jax.vmap(lambda single: jax.random.permutation(single, half_count))(perm_keys)
    flips = jax.random.randint(key_flip, (SEQS, half_count), 0, 2)
    first = jnp.where(flips == 1, NBLK - 1 - pairs, pairs)
    second = NBLK - 1 - first
    return jnp.stack([first, second], axis=2).reshape(SEQS, NBLK).astype(jnp.int32)


def with_spikes(values, stream_key, source, target, parts, factor):
    owner, partner = [(jnp.arange(values.shape[axis_at]) // (values.shape[axis_at] // parts)).reshape([-1 if axis == axis_at else 1 for axis in range(values.ndim)]) for axis_at in (source, target)]
    chosen = jax.random.permutation(stream_key, parts)[partner]
    strong = (owner == chosen) | (owner == (partner + parts // 2) % parts)
    return jnp.where(strong, factor * values, values)


def level_of(stream_key, extent, cuts, smallest, high):
    loudness = 1.0
    for axis_at, parts in cuts:
        steps = jax.random.uniform(jax.random.fold_in(jax.random.fold_in(stream_key, 6), axis_at), (parts,), jnp.float32, smallest / len(cuts), high / len(cuts))
        loudness = loudness * jnp.repeat(jnp.exp(steps), extent[axis_at] // parts).reshape((-1,) + (1,) * (len(extent) - 1 - axis_at))
    return loudness


def split_up(amount, total, reach, slope):
    loads = [(1 << 20) // math.isqrt(grade ** slope) + 1 for grade in range(2, amount + 1)]
    spare, holding = total - reach - (amount - 1), [1] * (amount - 1)
    while spare > 0:
        candidates = [i for i in range(amount - 1) if holding[i] < reach]
        whole, budget = sum([loads[i] for i in candidates]), spare
        for i in candidates:
            more = min(reach - holding[i], max(1, budget * loads[i] // whole), spare)
            holding[i] = holding[i] + more
            spare = spare - more
    return np.array([reach] + holding)


def uneven_parts(stream_key, count, total, limit, lean):
    if count == 2:
        one = jax.random.randint(stream_key, (), max(1, total - limit), min(limit, total - 1) + 1)
        return jnp.stack([one, total - one])
    lengths = jnp.asarray(split_up(count, total, limit, lean), jnp.int32)
    pairs = (count - 1) // 2
    source_of, taker = lengths[1:1 + 2 * pairs:2], lengths[2:2 + 2 * pairs:2]
    slack = jnp.minimum(source_of - 1, limit - taker)
    shifted = jax.random.randint(jax.random.fold_in(stream_key, 1), (pairs,), 0, 1 << 20) % (slack + 1)
    lengths = lengths.at[1:1 + 2 * pairs:2].set(source_of - shifted).at[2:2 + 2 * pairs:2].set(taker + shifted)
    return lengths[jax.random.permutation(jax.random.fold_in(stream_key, 2), count)]


def scatter_about(stream_key, extent, spread, limit, cuts=(), kind=jnp.bfloat16):
    values = spread * jax.random.normal(stream_key, extent, jnp.float32)
    if cuts:
        values = values * level_of(stream_key, extent, cuts, -0.22, 0.18)
    return jnp.clip(values, -limit, limit).astype(kind)


def heavy_noise(own_key, extent, spread, limit, shards, heavy, kind=jnp.bfloat16):
    values = spread * jax.random.normal(own_key, extent, jnp.float32)
    if shards:
        values = values * level_of(own_key, extent, shards, -0.22, 0.18)
    return jnp.clip(with_spikes(values, jax.random.fold_in(own_key, 3), *heavy), -limit, limit).astype(kind)


def setup_inputs(seed: int = 0) -> dict:
    seeds = jax.random.split(jax.random.key(seed), 14)
    return {
        "layer_input": draw_layer_input(jax.random.fold_in(seeds[13], 71), 0),
        "attn_gain": jnp.clip(1.0 + 0.1 * jax.random.normal(seeds[1], (D,), jnp.float32), 0.5, 1.5).astype(jnp.bfloat16),
        "w_query": scatter_about(seeds[2], (D, HEADS * HEAD_DIM), D ** -0.5, 0.125, ((1, 4),)),
        "w_key": scatter_about(seeds[3], (D, KV_HEADS * HEAD_DIM), D ** -0.5, 0.125, ((1, 4),)),
        "w_value": scatter_about(seeds[4], (D, KV_HEADS * HEAD_DIM), D ** -0.5, 0.125, ((1, 4),)),
        "w_out": scatter_about(seeds[5], (HEADS * HEAD_DIM, D), 4 ** -0.5, 3.0, ((0, 4),)),
        "ffn_gain": jnp.clip(1.0 + 0.1 * jax.random.normal(seeds[6], (D,), jnp.float32), 0.5, 1.5).astype(jnp.bfloat16),
        "w_gate": scatter_about(seeds[7], (D, FF), D ** -0.5, 0.125, ((1, 4),)),
        "w_up": scatter_about(seeds[8], (D, FF), D ** -0.5, 0.125, ((1, 4),)),
        "w_down": scatter_about(seeds[9], (FF, D), FF ** -0.5, 0.0625, ((0, 4),)),
        "cotangent": heavy_noise(seeds[10], (SEQS, LENGTH, D), 1.0, 6.0, ((1, 8),), (1, 2, 8, 2.0)),
        "block_ids": draw_block_ids(jax.random.fold_in(seeds[13], 71), 0),
        "doc_ids": jax.vmap(lambda own: jnp.searchsorted(jnp.cumsum(uneven_parts(own, 3, LENGTH, LENGTH // 2, 0)), jnp.arange(LENGTH), side="right"))(jax.random.split(seeds[12], SEQS)).reshape((SEQS, LENGTH)).astype(jnp.int32),
    }


EPS = 1e-05
ROPE_BASE = 500000.0
MASKED = -1e+30

def rope_angles(positions):
    half_dim = HEAD_DIM // 2
    freq = jnp.exp(jnp.arange(half_dim, dtype=jnp.float32) * (-2.0 * math.log(ROPE_BASE) / HEAD_DIM))
    angle = positions.astype(jnp.float32)[:, None] * freq[None, :]
    return (jnp.cos(angle)[:, None, :], jnp.sin(angle)[:, None, :])

def rotate(values, cosine, sine):
    half_dim = HEAD_DIM // 2
    first = values[..., :half_dim]
    second = values[..., half_dim:]
    return jnp.concatenate([first * cosine - second * sine, second * cosine + first * sine], axis=-1)

def norm_forward(values, gain):
    factor = lax.rsqrt(lax.optimization_barrier(jnp.mean(values * values, axis=-1, keepdims=True)) + EPS)
    unit = values * factor
    return (unit, factor, unit * gain.astype(jnp.float32))

def norm_backward(grad_out, unit, factor, gain):
    grad_gain = lax.optimization_barrier(jnp.sum(grad_out * unit, axis=0))
    scaled = grad_out * gain.astype(jnp.float32)
    grad_in = factor * (scaled - unit * lax.optimization_barrier(jnp.mean(scaled * unit, axis=-1, keepdims=True)))
    return (grad_in, grad_gain)

def barrier_round(values):
    return lax.optimization_barrier(values.astype(jnp.bfloat16)).astype(jnp.float32)

def masked_scores(query_f32, key_f32, query_pos, query_doc, key_pos, key_doc):
    scores = jnp.einsum('qhgd,khd->hgqk', query_f32, key_f32) * HEAD_DIM ** (-0.5)
    allowed = (key_pos[None, :] <= query_pos[:, None]) & (key_doc[None, :] == query_doc[:, None])
    return jnp.where(allowed[None, None], scores, MASKED)

def sequence_pass(input_seq, grad_seq, blocks, docs, weights):
    attn_gain, w_query, w_key, w_value, w_out, ffn_gain, w_gate, w_up, w_down = weights
    group = HEADS // KV_HEADS
    positions = (blocks[:, None] * BLK + jnp.arange(BLK, dtype=jnp.int32)[None, :]).reshape(LENGTH).astype(jnp.int32)
    pos_docs = jnp.take(docs, positions, axis=0)
    flat = input_seq.astype(jnp.float32)
    unit1, factor1, scaled1 = norm_forward(flat, attn_gain)
    normed1 = scaled1.astype(jnp.bfloat16)
    query = jnp.dot(normed1, w_query, preferred_element_type=jnp.float32).reshape(LENGTH, HEADS, HEAD_DIM)
    keys = jnp.dot(normed1, w_key, preferred_element_type=jnp.float32).reshape(LENGTH, KV_HEADS, HEAD_DIM)
    values = jnp.dot(normed1, w_value, preferred_element_type=jnp.float32).astype(jnp.bfloat16).reshape(LENGTH, KV_HEADS, HEAD_DIM)
    cosine, sine = rope_angles(positions)
    query_rot = rotate(query, cosine, sine).astype(jnp.bfloat16)
    key_rot = rotate(keys, cosine, sine).astype(jnp.bfloat16)
    key_f32 = key_rot.astype(jnp.float32)
    value_f32 = values.astype(jnp.float32)
    rows_per = math.gcd(LENGTH, 256)
    block_count = LENGTH // rows_per

    def split_rows(array):
        return array.reshape((block_count, rows_per) + array.shape[1:])

    def forward_block(carry, pieces):
        query_blk, pos_blk, doc_blk = pieces
        query_f32 = query_blk.astype(jnp.float32).reshape(rows_per, KV_HEADS, group, HEAD_DIM)
        scores = masked_scores(query_f32, key_f32, pos_blk, doc_blk, positions, pos_docs)
        top = lax.optimization_barrier(jnp.max(scores, axis=-1, keepdims=True))
        expd = jnp.exp(scores - top)
        total = lax.optimization_barrier(jnp.sum(expd, axis=-1, keepdims=True))
        probs = (expd / total).astype(jnp.bfloat16)
        result = jnp.einsum('hgqk,khd->qhgd', probs.astype(jnp.float32), value_f32)
        return (carry, (result.reshape(rows_per, HEADS, HEAD_DIM).astype(jnp.bfloat16), (top + jnp.log(total))[..., 0]))
    _, (attended, log_totals) = lax.scan(forward_block, jnp.zeros((), jnp.int32), (split_rows(query_rot), split_rows(positions), split_rows(pos_docs)))
    attended = attended.reshape(LENGTH, HEADS, HEAD_DIM)
    attended_flat = attended.reshape(LENGTH, HEADS * HEAD_DIM)
    hidden = flat + jnp.dot(attended_flat, w_out, preferred_element_type=jnp.float32)
    unit2, factor2, scaled2 = norm_forward(hidden, ffn_gain)
    normed2 = scaled2.astype(jnp.bfloat16)
    gate = jnp.dot(normed2, w_gate, preferred_element_type=jnp.float32)
    upper = jnp.dot(normed2, w_up, preferred_element_type=jnp.float32)
    sigma = jax.nn.sigmoid(gate)
    silu = gate * sigma
    act = (silu * upper).astype(jnp.bfloat16)
    out_seq = (hidden + jnp.dot(act, w_down, preferred_element_type=jnp.float32)).astype(jnp.bfloat16)
    grad_w_down = jnp.dot(act.T, grad_seq, preferred_element_type=jnp.float32)
    grad_act = jnp.dot(grad_seq, w_down.T, preferred_element_type=jnp.float32)
    grad_gate = (grad_act * upper * sigma * (1.0 + gate * (1.0 - sigma))).astype(jnp.bfloat16)
    grad_upper = (grad_act * silu).astype(jnp.bfloat16)
    grad_w_gate = jnp.dot(normed2.T, grad_gate, preferred_element_type=jnp.float32)
    grad_w_up = jnp.dot(normed2.T, grad_upper, preferred_element_type=jnp.float32)
    grad_normed2 = jnp.dot(grad_gate, w_gate.T, preferred_element_type=jnp.float32) + jnp.dot(grad_upper, w_up.T, preferred_element_type=jnp.float32)
    grad_hnorm, grad_ffn_gain = norm_backward(grad_normed2, unit2, factor2, ffn_gain)
    grad_hidden = grad_seq.astype(jnp.float32) + grad_hnorm
    grad_hidden_b = grad_hidden.astype(jnp.bfloat16)
    grad_w_out = jnp.dot(attended_flat.T, grad_hidden_b, preferred_element_type=jnp.float32)
    grad_attended = jnp.dot(grad_hidden_b, w_out.T, preferred_element_type=jnp.float32).astype(jnp.bfloat16).reshape(LENGTH, HEADS, HEAD_DIM)
    delta = lax.optimization_barrier(jnp.sum(grad_attended.astype(jnp.float32) * attended.astype(jnp.float32), axis=-1))
    scale = HEAD_DIM ** (-0.5)

    def backward_block(carry, pieces):
        grad_keys, grad_values = carry
        query_blk, grad_blk, delta_blk, lse_blk, pos_blk, doc_blk = pieces
        query_f32 = query_blk.astype(jnp.float32).reshape(rows_per, KV_HEADS, group, HEAD_DIM)
        grad_f32 = grad_blk.astype(jnp.float32).reshape(rows_per, KV_HEADS, group, HEAD_DIM)
        scores = masked_scores(query_f32, key_f32, pos_blk, doc_blk, positions, pos_docs)
        probs = jnp.exp(scores - lse_blk[..., None])
        delta_t = jnp.transpose(delta_blk.reshape(rows_per, KV_HEADS, group), (1, 2, 0))
        grad_probs = jnp.einsum('qhgd,khd->hgqk', grad_f32, value_f32)
        grad_scores = barrier_round(probs * (grad_probs - delta_t[..., None]))
        grad_query = jnp.einsum('hgqk,khd->qhgd', grad_scores, key_f32) * scale
        grad_keys = grad_keys + jnp.einsum('hgqk,qhgd->khd', grad_scores, query_f32) * scale
        grad_values = grad_values + jnp.einsum('hgqk,qhgd->khd', barrier_round(probs), grad_f32)
        return ((grad_keys, grad_values), grad_query.reshape(rows_per, HEADS, HEAD_DIM))
    zero_kv = jnp.zeros((LENGTH, KV_HEADS, HEAD_DIM), jnp.float32)
    (grad_key_rot, grad_values), grad_query_rot = lax.scan(backward_block, (zero_kv, zero_kv), (split_rows(query_rot), split_rows(grad_attended), split_rows(delta), log_totals, split_rows(positions), split_rows(pos_docs)))
    grad_query = rotate(grad_query_rot.reshape(LENGTH, HEADS, HEAD_DIM), cosine, -sine).astype(jnp.bfloat16).reshape(LENGTH, HEADS * HEAD_DIM)
    grad_keys = rotate(grad_key_rot, cosine, -sine).astype(jnp.bfloat16).reshape(LENGTH, KV_HEADS * HEAD_DIM)
    grad_values_b = grad_values.astype(jnp.bfloat16).reshape(LENGTH, KV_HEADS * HEAD_DIM)
    grad_w_query = jnp.dot(normed1.T, grad_query, preferred_element_type=jnp.float32)
    grad_w_key = jnp.dot(normed1.T, grad_keys, preferred_element_type=jnp.float32)
    grad_w_value = jnp.dot(normed1.T, grad_values_b, preferred_element_type=jnp.float32)
    grad_normed1 = jnp.dot(grad_query, w_query.T, preferred_element_type=jnp.float32) + jnp.dot(grad_keys, w_key.T, preferred_element_type=jnp.float32) + jnp.dot(grad_values_b, w_value.T, preferred_element_type=jnp.float32)
    grad_xnorm, grad_attn_gain = norm_backward(grad_normed1, unit1, factor1, attn_gain)
    grad_input_seq = grad_hidden + grad_xnorm
    grads = (grad_attn_gain, grad_w_query, grad_w_key, grad_w_value, grad_w_out, grad_ffn_gain, grad_w_gate, grad_w_up, grad_w_down)
    return (out_seq, grad_input_seq, grads)

def reference(layer_input, attn_gain, w_query, w_key, w_value, w_out, ffn_gain, w_gate, w_up, w_down, cotangent, block_ids, doc_ids):
    weights = (attn_gain, w_query, w_key, w_value, w_out, ffn_gain, w_gate, w_up, w_down)
    zeros = tuple((jnp.zeros(weight.shape, jnp.float32) for weight in weights))

    def step_seq(carry, pieces):
        out_seq, grad_input_seq, grads = sequence_pass(pieces[0], pieces[1], pieces[2], pieces[3], weights)
        return (tuple((total + part for total, part in zip(carry, grads))), (out_seq, grad_input_seq))
    totals, (block_out, grad_input) = lax.scan(step_seq, zeros, (layer_input, cotangent, block_ids, doc_ids))
    return (block_out, grad_input, totals[0], totals[1], totals[2], totals[3], totals[4], totals[5], totals[6], totals[7], totals[8])
```

```python
import functools
import math

import jax
import jax.numpy as jnp
from jax import lax
from jax.experimental import pallas as pl
from jax.experimental.pallas import tpu as pltpu
from jax.sharding import PartitionSpec as P

HEAD_DIM = 64
HALF = HEAD_DIM // 2
EPS = 1e-05
ROPE_BASE = 500000.0
MASKED = -1e30
BF16 = jnp.bfloat16
F32 = jnp.float32


def heads_of(ref, head, group):
    return jnp.concatenate(
        [
            ref[0, (head * group + j) * HEAD_DIM : (head * group + j + 1) * HEAD_DIM, :]
            for j in range(group)
        ],
        axis=1,
    )


def key_tile(slot_ref, seq, block, halves):
    slot = slot_ref[seq, block]
    return (slot // 2) * halves + seq * 2 + slot % 2


def allowed_keys(block, keys, bounds, group):
    key_pos = block * keys + lax.broadcasted_iota(jnp.int32, (keys, keys), 0)
    ok = (key_pos >= bounds[0:1, :]) & (key_pos <= bounds[1:2, :])
    bias = jnp.where(ok, 0.0, MASKED).astype(F32)
    return jnp.concatenate([bias] * group, axis=1)


def forward_kernel(kv_heads, group, slot_ref, own_ref, low_ref, q_ref, kv_ref, bound_ref, att_ref, lse_ref):
    which = pl.program_id(0)
    halves = pl.num_programs(0)
    seq = which // 2
    keys = kv_ref.shape[2]
    width = group * keys
    queries = [heads_of(q_ref, g, group) for g in range(kv_heads)]
    bounds = bound_ref[0]

    def step(block, carry):
        tile = key_tile(slot_ref, seq, block, halves)
        bias = allowed_keys(block, keys, bounds, group)
        out = []
        for g in range(kv_heads):
            top, total, acc = carry[g]
            key_t = kv_ref[tile, g * HEAD_DIM : (g + 1) * HEAD_DIM, :]
            value_t = kv_ref[tile, (kv_heads + g) * HEAD_DIM : (kv_heads + g + 1) * HEAD_DIM, :]
            scores = lax.dot_general(
                key_t, queries[g], (((0,), (0,)), ((), ())), preferred_element_type=F32
            )
            scores = jnp.where(bias < 0.0, MASKED, scores)
            new_top = jnp.maximum(top, jnp.max(scores, axis=0, keepdims=True))
            shrink = jnp.exp(top - new_top)
            probs = jnp.exp(scores - new_top)
            total = total * shrink + jnp.sum(probs, axis=0, keepdims=True)
            acc = acc * shrink + jnp.dot(value_t, probs.astype(BF16), preferred_element_type=F32)
            out.append((new_top, total, acc))
        return tuple(out)

    start = tuple(
        (
            jnp.full((1, width), MASKED, F32),
            jnp.zeros((1, width), F32),
            jnp.zeros((HEAD_DIM, width), F32),
        )
        for _ in range(kv_heads)
    )
    final = lax.fori_loop(low_ref[which], own_ref[which] + 1, step, start)
    for g in range(kv_heads):
        top, total, acc = final[g]
        lse_ref[0, g : g + 1, :] = top + jnp.log(total)
        result = (acc / total).astype(BF16)
        for j in range(group):
            att_ref[0, (g * group + j) * HEAD_DIM : (g * group + j + 1) * HEAD_DIM, :] = result[
                :, j * keys : (j + 1) * keys
            ]


def backward_kernel(
    kv_heads, group, slot_ref, own_ref, low_ref, q_ref, kv_ref, bound_ref, att_ref, lse_ref, do_ref, dq_ref, dkv_ref, total_ref
):
    which = pl.program_id(0)
    halves = pl.num_programs(0)
    seq = which // 2
    keys = kv_ref.shape[2]
    width = group * keys

    @pl.when(which == 0)
    def _():
        total_ref[...] = jnp.zeros_like(total_ref)

    queries = [heads_of(q_ref, g, group) for g in range(kv_heads)]
    grads = [heads_of(do_ref, g, group) for g in range(kv_heads)]
    deltas = [
        jnp.sum(grads[g].astype(F32) * heads_of(att_ref, g, group).astype(F32), axis=0, keepdims=True)
        for g in range(kv_heads)
    ]
    bounds = bound_ref[0]
    contract_last = (((1,), (1,)), ((), ()))

    def step(block, carry):
        tile = key_tile(slot_ref, seq, block, halves)
        bias = allowed_keys(block, keys, bounds, group)
        out = []
        for g in range(kv_heads):
            k_rows = slice(g * HEAD_DIM, (g + 1) * HEAD_DIM)
            v_rows = slice((kv_heads + g) * HEAD_DIM, (kv_heads + g + 1) * HEAD_DIM)
            key_t = kv_ref[tile, k_rows, :]
            value_t = kv_ref[tile, v_rows, :]
            scores = lax.dot_general(
                key_t, queries[g], (((0,), (0,)), ((), ())), preferred_element_type=F32
            )
            scores = jnp.where(bias < 0.0, MASKED, scores)
            probs = jnp.exp(scores - lse_ref[0, g : g + 1, :])
            grad_probs = lax.dot_general(
                value_t, grads[g], (((0,), (0,)), ((), ())), preferred_element_type=F32
            )
            grad_scores = (probs * (grad_probs - deltas[g])).astype(BF16)
            out.append(carry[g] + jnp.dot(key_t, grad_scores, preferred_element_type=F32))
            total_ref[tile, k_rows, :] += lax.dot_general(
                queries[g], grad_scores, contract_last, preferred_element_type=F32
            )
            total_ref[tile, v_rows, :] += lax.dot_general(
                grads[g], probs.astype(BF16), contract_last, preferred_element_type=F32
            )
        return tuple(out)

    start = tuple(jnp.zeros((HEAD_DIM, width), F32) for _ in range(kv_heads))
    final = lax.fori_loop(low_ref[which], own_ref[which] + 1, step, start)
    for g in range(kv_heads):
        for j in range(group):
            dq_ref[0, (g * group + j) * HEAD_DIM : (g * group + j + 1) * HEAD_DIM, :] = final[g][
                :, j * keys : (j + 1) * keys
            ]

    @pl.when(which == halves - 1)
    def _():
        dkv_ref[...] = total_ref[...].astype(BF16)


def tile_spec(shape):
    return pl.BlockSpec((1,) + shape[1:], lambda i, *_: (i,) + (0,) * (len(shape) - 1))


def whole_spec(shape):
    return pl.BlockSpec(shape, lambda i, *_: (0,) * len(shape))


def attend_forward(slots, own, low, q_t, kv_all, bounds, kv_heads, group):
    halves, width, keys = q_t.shape
    lse_shape = (halves, kv_heads, group * keys)
    return pl.pallas_call(
        functools.partial(forward_kernel, kv_heads, group),
        out_shape=(jax.ShapeDtypeStruct(q_t.shape, BF16), jax.ShapeDtypeStruct(lse_shape, F32)),
        grid_spec=pltpu.PrefetchScalarGridSpec(
            num_scalar_prefetch=3,
            grid=(halves,),
            in_specs=[tile_spec(q_t.shape), whole_spec(kv_all.shape), tile_spec(bounds.shape)],
            out_specs=(tile_spec(q_t.shape), tile_spec(lse_shape)),
        ),
        cost_estimate=pl.CostEstimate(flops=2_000_000_000, bytes_accessed=8_000_000, transcendentals=4_000_000),
        name="attend_forward",
    )(slots, own, low, q_t, kv_all, bounds)


def attend_backward(slots, own, low, q_t, kv_all, bounds, att_t, lse, do_t, kv_heads, group):
    halves, width, keys = q_t.shape
    return pl.pallas_call(
        functools.partial(backward_kernel, kv_heads, group),
        out_shape=(jax.ShapeDtypeStruct(q_t.shape, F32), jax.ShapeDtypeStruct(kv_all.shape, BF16)),
        grid_spec=pltpu.PrefetchScalarGridSpec(
            num_scalar_prefetch=3,
            grid=(halves,),
            in_specs=[
                tile_spec(q_t.shape),
                whole_spec(kv_all.shape),
                tile_spec(bounds.shape),
                tile_spec(att_t.shape),
                tile_spec(lse.shape),
                tile_spec(do_t.shape),
            ],
            out_specs=(tile_spec(q_t.shape), whole_spec(kv_all.shape)),
            scratch_shapes=[pltpu.VMEM(kv_all.shape, F32)],
        ),
        cost_estimate=pl.CostEstimate(flops=5_000_000_000, bytes_accessed=12_000_000, transcendentals=4_000_000),
        name="attend_backward",
    )(slots, own, low, q_t, kv_all, bounds, att_t, lse, do_t)


def sum_bf16(*terms):
    total = terms[0].astype(F32)
    for term in terms[1:]:
        total = total + term.astype(F32)
    return total.astype(BF16)


def swap(array, axis, bit, count):
    return lax.ppermute(array, axis, [(i, i ^ bit) for i in range(count)])


def sum_over_tp(part, core, tp_count):
    rows = part.shape[0] // 2
    mine = lax.dynamic_slice_in_dim(part, core * rows, rows, 0)
    theirs = lax.dynamic_slice_in_dim(part, (1 - core) * rows, rows, 0)
    half = sum_bf16(mine, swap(theirs, "tp", 1, tp_count))
    bit = 2
    while bit < tp_count:
        half = sum_bf16(half, swap(half, "tp", bit, tp_count))
        bit *= 2
    other = swap(half, "tp", 1, tp_count)
    both = jnp.where(core == 0, jnp.stack([half, other]), jnp.stack([other, half]))
    return both.reshape(part.shape)


def line_scatter(part, axis, line, line_count):
    def entry(index):
        return lax.dynamic_index_in_dim(
            part, jnp.clip(index, 0, line_count - 1), axis, keepdims=False
        )

    up = down = None
    for step in range(1, line_count):
        send_up = entry(line_count - step + line)
        send_down = entry(step - line_count + line)
        if up is not None:
            send_up = sum_bf16(send_up, up)
            send_down = sum_bf16(send_down, down)
        last = line_count - 1
        up = lax.ppermute(
            send_up, "ctx", [(2 * i + x, 2 * i + 2 + x) for i in range(step) for x in range(2)]
        )
        down = lax.ppermute(
            send_down,
            "ctx",
            [(2 * (last - i) + x, 2 * (last - i) - 2 + x) for i in range(step) for x in range(2)],
        )
    total = entry(line).astype(F32)
    if up is not None:
        total = total + up.astype(F32) + down.astype(F32)
    return total


def rope_table(positions):
    freq = jnp.exp(jnp.arange(HALF, dtype=F32) * (-2.0 * math.log(ROPE_BASE) / HEAD_DIM))
    angle = positions.astype(F32)[:, None, :] * freq[None, :, None]
    return jnp.cos(angle)[:, None], jnp.sin(angle)[:, None]


def rotate_t(values, cosine, sine):
    halves, width, keys = values.shape
    split = values.reshape(halves, width // HEAD_DIM, 2, HALF, keys)
    first, second = split[:, :, 0], split[:, :, 1]
    return jnp.stack(
        [first * cosine - second * sine, second * cosine + first * sine], axis=2
    ).reshape(values.shape)


def norm_forward(values, gain):
    factor = lax.rsqrt(jnp.mean(values * values, axis=-1, keepdims=True) + EPS)
    unit = values * factor
    return unit, factor, unit * gain.astype(F32)


def norm_backward(grad_out, unit, factor, gain):
    grad_gain = jnp.sum(grad_out * unit, axis=0)
    scaled = grad_out * gain.astype(F32)
    grad_in = factor * (scaled - unit * jnp.mean(scaled * unit, axis=-1, keepdims=True))
    return grad_in, grad_gain


def on_device(
    ctx_count,
    tp_count,
    layer_input,
    attn_gain,
    w_query,
    w_key,
    w_value,
    w_out,
    ffn_gain,
    w_gate,
    w_up,
    w_down,
    cotangent,
    block_ids,
    doc_ids,
):
    seqs, rows, width = layer_input.shape
    block_len = rows // 2
    halves = seqs * 2
    length = doc_ids.shape[1]
    block_total = block_ids.shape[1]
    q_width, kv_width = w_query.shape[1], w_key.shape[1]
    kv_heads = kv_width // HEAD_DIM
    group = q_width // kv_width
    tokens = seqs * rows
    share = width // ctx_count
    place = lax.axis_index("ctx")
    line_count = ctx_count // 2
    line, side = place // 2, place % 2
    core = lax.axis_index("tp") % 2

    def pair(array):
        return swap(array, "ctx", 1, ctx_count)

    def of_side(array, which):
        split = array.reshape(tokens, line_count, 2, share)
        return lax.dynamic_index_in_dim(split, which, 2, keepdims=False)

    def both_tokens(array):
        return jnp.concatenate([array, pair(array)], axis=0)

    def side_columns(array):
        return jnp.concatenate([of_side(array, side), pair(of_side(array, 1 - side))], axis=0)

    def weight_rows(columns, grads):
        part = lax.dot_general(
            columns, grads, (((0,), (0,)), ((), ())), preferred_element_type=F32
        ).astype(BF16)
        return line_scatter(part, 0, line, line_count)

    def weight_columns(acts, columns):
        part = lax.dot_general(
            acts, columns, (((0,), (0,)), ((), ())), preferred_element_type=F32
        ).astype(BF16)
        return line_scatter(part, 1, line, line_count)

    slot_index = jnp.arange(block_total, dtype=jnp.int32)
    slots = jnp.sum(
        jnp.where(block_ids[:, :, None] == slot_index[None, None, :], slot_index[None, :, None], 0),
        axis=1,
    )
    own_blocks = lax.dynamic_slice_in_dim(block_ids, 2 * place, 2, 1).reshape(halves)
    positions = own_blocks[:, None] * block_len + jnp.arange(block_len, dtype=jnp.int32)[None, :]
    split_pos = positions.reshape(seqs, rows)
    docs = jnp.take_along_axis(doc_ids, split_pos, axis=1)
    first_key = jnp.sum((doc_ids[:, :, None] < docs[:, None, :]).astype(jnp.int32), axis=1).reshape(
        halves, block_len
    )
    bounds = jnp.stack([first_key, positions], axis=1)
    low_blocks = first_key[:, 0] // block_len
    cosine, sine = rope_table(positions)

    flat_input = layer_input.reshape(tokens, width).astype(F32)
    unit1, factor1, scaled1 = norm_forward(flat_input, attn_gain)
    normed1 = scaled1.astype(BF16)
    tiles1 = normed1.reshape(halves, block_len, width)

    def project_t(weight):
        return jnp.einsum("dc,htd->hct", weight, tiles1, preferred_element_type=F32)

    key_t = rotate_t(project_t(w_key), cosine, sine).astype(BF16)
    value_t = project_t(w_value).astype(BF16)
    kv_own = jnp.concatenate([key_t, value_t], axis=1)
    kv_all = lax.all_gather(kv_own, "ctx", axis=0, tiled=True)
    scale = HEAD_DIM ** (-0.5)
    query_t = (rotate_t(project_t(w_query), cosine, sine)).astype(BF16) * jnp.asarray(scale, BF16)
    grad_output = cotangent.reshape(tokens, width)
    grad_act = jnp.einsum("td,fd->tf", grad_output, w_down, preferred_element_type=F32)
    cot_side = side_columns(grad_output)
    normed1_side = side_columns(normed1)
    att_t, lse = attend_forward(
        slots, own_blocks, low_blocks, query_t, kv_all, bounds, kv_heads, group
    )
    attended = jnp.transpose(att_t, (0, 2, 1)).reshape(tokens, q_width)
    attn_part = jnp.dot(attended, w_out, preferred_element_type=F32).astype(BF16)
    hidden = flat_input + sum_over_tp(attn_part, core, tp_count).astype(F32)

    unit2, factor2, scaled2 = norm_forward(hidden, ffn_gain)
    normed2 = scaled2.astype(BF16)
    gate = jnp.dot(normed2, w_gate, preferred_element_type=F32)
    upper = jnp.dot(normed2, w_up, preferred_element_type=F32)
    sigma = jax.nn.sigmoid(gate)
    silu = gate * sigma
    act = (silu * upper).astype(BF16)
    grad_gate = (grad_act * upper * sigma * (1.0 + gate * (1.0 - sigma))).astype(BF16)
    grad_upper = (grad_act * silu).astype(BF16)
    grad_n2_part = (
        jnp.einsum("tf,df->td", grad_gate, w_gate, preferred_element_type=F32)
        + jnp.einsum("tf,df->td", grad_upper, w_up, preferred_element_type=F32)
    ).astype(BF16)
    grad_normed2 = sum_over_tp(grad_n2_part, core, tp_count).astype(F32)
    grad_w_down = weight_columns(both_tokens(act), cot_side)
    normed2_side = side_columns(normed2)
    grad_w_gate = weight_rows(normed2_side, both_tokens(grad_gate))
    grad_w_up = weight_rows(normed2_side, both_tokens(grad_upper))
    ffn_part = jnp.dot(act, w_down, preferred_element_type=F32).astype(BF16)
    block_out = (
        (hidden + sum_over_tp(ffn_part, core, tp_count).astype(F32))
        .astype(BF16)
        .reshape(seqs, rows, width)
    )
    grad_hnorm, grad_ffn_gain = norm_backward(grad_normed2, unit2, factor2, ffn_gain)
    grad_hidden = grad_output.astype(F32) + grad_hnorm
    grad_hidden_b = grad_hidden.astype(BF16)

    do_t = jnp.einsum(
        "cd,htd->hct",
        w_out,
        grad_hidden_b.reshape(halves, block_len, width),
        preferred_element_type=F32,
    ).astype(BF16)
    dq_t, dkv_part = attend_backward(
        slots, own_blocks, low_blocks, query_t, kv_all, bounds, att_t, lse, do_t, kv_heads, group
    )
    grad_w_out = weight_columns(both_tokens(attended), side_columns(grad_hidden_b))
    dkv_split = dkv_part.reshape((line_count, 2) + kv_own.shape)
    dkv_mine = lax.dynamic_index_in_dim(dkv_split, side, 1, keepdims=False)
    dkv_theirs = lax.dynamic_index_in_dim(dkv_split, 1 - side, 1, keepdims=False)
    dkv = line_scatter(sum_bf16(dkv_mine, pair(dkv_theirs)), 0, line, line_count)
    grad_query_t = (rotate_t(dq_t, cosine, -sine) * scale).astype(BF16)
    grad_key_t = rotate_t(dkv[:, :kv_width], cosine, -sine).astype(BF16)
    grad_value_t = dkv[:, kv_width:].astype(BF16)

    def to_rows(array):
        return jnp.transpose(array, (0, 2, 1)).reshape(tokens, array.shape[1])

    grad_query = to_rows(grad_query_t)
    grad_kv = to_rows(jnp.concatenate([grad_key_t, grad_value_t], axis=1))
    w_kv = jnp.concatenate([w_key, w_value], axis=1)
    grad_n1_part = (
        jnp.einsum("tc,dc->td", grad_query, w_query, preferred_element_type=F32)
        + jnp.einsum("tc,dc->td", grad_kv, w_kv, preferred_element_type=F32)
    ).astype(BF16)
    grad_normed1 = sum_over_tp(grad_n1_part, core, tp_count).astype(F32)
    grad_w_query = weight_rows(normed1_side, both_tokens(grad_query))
    grad_w_kv = weight_rows(normed1_side, both_tokens(grad_kv))
    grad_xnorm, grad_attn_gain = norm_backward(grad_normed1, unit1, factor1, attn_gain)
    grad_input = (grad_hidden + grad_xnorm).reshape(seqs, rows, width)
    gains = jnp.stack([grad_attn_gain, grad_ffn_gain]).reshape(2, ctx_count, share)
    gains = jnp.sum(lax.all_to_all(gains, "ctx", 1, 1, tiled=True), axis=1)
    return (
        block_out,
        grad_input,
        gains[0],
        grad_w_query,
        grad_w_kv[:, :kv_width],
        grad_w_kv[:, kv_width:],
        grad_w_out,
        gains[1],
        grad_w_gate,
        grad_w_up,
        grad_w_down,
    )


def solution(mesh):
    in_specs = (
        P(None, "ctx", None),
        P(),
        P(None, "tp"),
        P(None, "tp"),
        P(None, "tp"),
        P("tp", None),
        P(),
        P(None, "tp"),
        P(None, "tp"),
        P("tp", None),
        P(None, "ctx", None),
        P(),
        P(),
    )
    out_specs = (
        P(None, "ctx", None),
        P(None, "ctx", None),
        P("ctx"),
        P("ctx", "tp"),
        P("ctx", "tp"),
        P("ctx", "tp"),
        P("tp", "ctx"),
        P("ctx"),
        P("ctx", "tp"),
        P("ctx", "tp"),
        P("tp", "ctx"),
    )
    return jax.shard_map(
        functools.partial(on_device, mesh.shape["ctx"], mesh.shape["tp"]),
        mesh=mesh,
        in_specs=in_specs,
        out_specs=out_specs,
        check_vma=False,
    )
```

```python
import functools
import math

import jax
import jax.numpy as jnp
from jax import lax
from jax.experimental import pallas as pl
from jax.experimental.pallas import tpu as pltpu
from jax.sharding import PartitionSpec as P

HEAD_DIM = 64
HALF = HEAD_DIM // 2
EPS = 1e-05
ROPE_BASE = 500000.0
MASKED = -1e30
BF16 = jnp.bfloat16
F32 = jnp.float32


def heads_of(ref, head, group):
    return jnp.concatenate(
        [
            ref[0, (head * group + j) * HEAD_DIM : (head * group + j + 1) * HEAD_DIM, :]
            for j in range(group)
        ],
        axis=1,
    )


def key_tile(slot_ref, seq, block, halves):
    slot = slot_ref[seq, block]
    return (slot // 2) * halves + seq * 2 + slot % 2


def allowed_keys(block, keys, bounds, group):
    key_pos = block * keys + lax.broadcasted_iota(jnp.int32, (keys, keys), 0)
    ok = (key_pos >= bounds[0:1, :]) & (key_pos <= bounds[1:2, :])
    bias = jnp.where(ok, 0.0, MASKED).astype(F32)
    return jnp.concatenate([bias] * group, axis=1)


def forward_kernel(kv_heads, group, slot_ref, own_ref, low_ref, q_ref, kv_ref, bound_ref, att_ref, lse_ref):
    which = pl.program_id(0)
    halves = pl.num_programs(0)
    seq = which // 2
    keys = kv_ref.shape[2]
    width = group * keys
    queries = [heads_of(q_ref, g, group) for g in range(kv_heads)]
    bounds = bound_ref[0]

    def step(block, carry):
        tile = key_tile(slot_ref, seq, block, halves)
        bias = allowed_keys(block, keys, bounds, group)
        out = []
        for g in range(kv_heads):
            top, total, acc = carry[g]
            key_t = kv_ref[tile, g * HEAD_DIM : (g + 1) * HEAD_DIM, :]
            value_t = kv_ref[tile, (kv_heads + g) * HEAD_DIM : (kv_heads + g + 1) * HEAD_DIM, :]
            scores = lax.dot_general(
                key_t, queries[g], (((0,), (0,)), ((), ())), preferred_element_type=F32
            )
            scores = jnp.where(bias < 0.0, MASKED, scores)
            new_top = jnp.maximum(top, jnp.max(scores, axis=0, keepdims=True))
            shrink = jnp.exp(top - new_top)
            probs = jnp.exp(scores - new_top)
            total = total * shrink + jnp.sum(probs, axis=0, keepdims=True)
            acc = acc * shrink + jnp.dot(value_t, probs.astype(BF16), preferred_element_type=F32)
            out.append((new_top, total, acc))
        return tuple(out)

    start = tuple(
        (
            jnp.full((1, width), MASKED, F32),
            jnp.zeros((1, width), F32),
            jnp.zeros((HEAD_DIM, width), F32),
        )
        for _ in range(kv_heads)
    )
    final = lax.fori_loop(low_ref[which], own_ref[which] + 1, step, start)
    for g in range(kv_heads):
        top, total, acc = final[g]
        lse_ref[0, g : g + 1, :] = top + jnp.log(total)
        result = (acc / total).astype(BF16)
        for j in range(group):
            att_ref[0, (g * group + j) * HEAD_DIM : (g * group + j + 1) * HEAD_DIM, :] = result[
                :, j * keys : (j + 1) * keys
            ]


def backward_kernel(
    kv_heads, group, slot_ref, own_ref, low_ref, q_ref, kv_ref, bound_ref, att_ref, lse_ref, do_ref, dq_ref, dkv_ref, total_ref
):
    which = pl.program_id(0)
    halves = pl.num_programs(0)
    seq = which // 2
    keys = kv_ref.shape[2]
    width = group * keys

    @pl.when(which == 0)
    def _():
        total_ref[...] = jnp.zeros_like(total_ref)

    queries = [heads_of(q_ref, g, group) for g in range(kv_heads)]
    grads = [heads_of(do_ref, g, group) for g in range(kv_heads)]
    deltas = [
        jnp.sum(grads[g].astype(F32) * heads_of(att_ref, g, group).astype(F32), axis=0, keepdims=True)
        for g in range(kv_heads)
    ]
    bounds = bound_ref[0]
    contract_last = (((1,), (1,)), ((), ()))

    def step(block, carry):
        tile = key_tile(slot_ref, seq, block, halves)
        bias = allowed_keys(block, keys, bounds, group)
        out = []
        for g in range(kv_heads):
            k_rows = slice(g * HEAD_DIM, (g + 1) * HEAD_DIM)
            v_rows = slice((kv_heads + g) * HEAD_DIM, (kv_heads + g + 1) * HEAD_DIM)
            key_t = kv_ref[tile, k_rows, :]
            value_t = kv_ref[tile, v_rows, :]
            scores = lax.dot_general(
                key_t, queries[g], (((0,), (0,)), ((), ())), preferred_element_type=F32
            )
            scores = jnp.where(bias < 0.0, MASKED, scores)
            probs = jnp.exp(scores - lse_ref[0, g : g + 1, :])
            grad_probs = lax.dot_general(
                value_t, grads[g], (((0,), (0,)), ((), ())), preferred_element_type=F32
            )
            grad_scores = (probs * (grad_probs - deltas[g])).astype(BF16)
            out.append(carry[g] + jnp.dot(key_t, grad_scores, preferred_element_type=F32))
            total_ref[tile, k_rows, :] += lax.dot_general(
                queries[g], grad_scores, contract_last, preferred_element_type=F32
            )
            total_ref[tile, v_rows, :] += lax.dot_general(
                grads[g], probs.astype(BF16), contract_last, preferred_element_type=F32
            )
        return tuple(out)

    start = tuple(jnp.zeros((HEAD_DIM, width), F32) for _ in range(kv_heads))
    final = lax.fori_loop(low_ref[which], own_ref[which] + 1, step, start)
    for g in range(kv_heads):
        for j in range(group):
            dq_ref[0, (g * group + j) * HEAD_DIM : (g * group + j + 1) * HEAD_DIM, :] = final[g][
                :, j * keys : (j + 1) * keys
            ]

    @pl.when(which == halves - 1)
    def _():
        dkv_ref[...] = total_ref[...].astype(BF16)


def tile_spec(shape):
    return pl.BlockSpec((1,) + shape[1:], lambda i, *_: (i,) + (0,) * (len(shape) - 1))


def whole_spec(shape):
    return pl.BlockSpec(shape, lambda i, *_: (0,) * len(shape))


def attend_forward(slots, own, low, q_t, kv_all, bounds, kv_heads, group):
    halves, width, keys = q_t.shape
    lse_shape = (halves, kv_heads, group * keys)
    return pl.pallas_call(
        functools.partial(forward_kernel, kv_heads, group),
        out_shape=(jax.ShapeDtypeStruct(q_t.shape, BF16), jax.ShapeDtypeStruct(lse_shape, F32)),
        grid_spec=pltpu.PrefetchScalarGridSpec(
            num_scalar_prefetch=3,
            grid=(halves,),
            in_specs=[tile_spec(q_t.shape), whole_spec(kv_all.shape), tile_spec(bounds.shape)],
            out_specs=(tile_spec(q_t.shape), tile_spec(lse_shape)),
        ),
        cost_estimate=pl.CostEstimate(flops=2_000_000_000, bytes_accessed=8_000_000, transcendentals=4_000_000),
        name="attend_forward",
    )(slots, own, low, q_t, kv_all, bounds)


def attend_backward(slots, own, low, q_t, kv_all, bounds, att_t, lse, do_t, kv_heads, group):
    halves, width, keys = q_t.shape
    return pl.pallas_call(
        functools.partial(backward_kernel, kv_heads, group),
        out_shape=(jax.ShapeDtypeStruct(q_t.shape, F32), jax.ShapeDtypeStruct(kv_all.shape, BF16)),
        grid_spec=pltpu.PrefetchScalarGridSpec(
            num_scalar_prefetch=3,
            grid=(halves,),
            in_specs=[
                tile_spec(q_t.shape),
                whole_spec(kv_all.shape),
                tile_spec(bounds.shape),
                tile_spec(att_t.shape),
                tile_spec(lse.shape),
                tile_spec(do_t.shape),
            ],
            out_specs=(tile_spec(q_t.shape), whole_spec(kv_all.shape)),
            scratch_shapes=[pltpu.VMEM(kv_all.shape, F32)],
        ),
        cost_estimate=pl.CostEstimate(flops=5_000_000_000, bytes_accessed=12_000_000, transcendentals=4_000_000),
        name="attend_backward",
    )(slots, own, low, q_t, kv_all, bounds, att_t, lse, do_t)


def column_spec(rows, share, column):
    if share % 128 == 0:
        return pl.BlockSpec((rows, share), lambda i, at: (0, column(i, at)))
    return pl.BlockSpec((None, rows, share), lambda i, at: (column(i, at), 0, 0))


def by_shares(array, share):
    if share % 128 == 0:
        return array
    return jnp.transpose(array.reshape(array.shape[0], -1, share), (1, 0, 2))


def copy_kernel(at_ref, in_ref, out_ref):
    out_ref[...] = in_ref[...]


def pick_columns(at, array, share, line_count):
    rows = array.shape[0]
    if share % 128 == 0:
        shape = (rows, line_count * share)
    else:
        shape = (line_count, rows, share)
    return pl.pallas_call(
        copy_kernel,
        out_shape=jax.ShapeDtypeStruct(shape, array.dtype),
        grid_spec=pltpu.PrefetchScalarGridSpec(
            num_scalar_prefetch=1,
            grid=(line_count,),
            in_specs=[column_spec(rows, share, lambda i, at: 2 * i + 1 - at[1])],
            out_specs=column_spec(rows, share, lambda i, at: i),
        ),
        cost_estimate=pl.CostEstimate(flops=0, bytes_accessed=4 * array.size, transcendentals=0),
        name="pick_columns",
    )(at, by_shares(array, share))


def product_kernel(count, at_ref, *refs):
    ins, outs, turned = refs[: 2 * count + 2], refs[2 * count + 2 : -1], refs[-1]
    own_ref, other_ref = ins[2 * count :]
    rows = own_ref.shape[0]

    @pl.when(pl.program_id(0) == 0)
    def _():
        for k in range(count):
            turned[k, :, :rows] = ins[2 * k][...].T
            turned[k, :, rows:] = ins[2 * k + 1][...].T

    for k in range(count):
        outs[k][...] = (
            jnp.dot(turned[k, :, :rows], own_ref[...], preferred_element_type=F32)
            + jnp.dot(turned[k, :, rows:], other_ref[...], preferred_element_type=F32)
        ).astype(BF16)


def product(at, own_columns, other_columns, own, other, offsets, share, line_count):
    rows, out_width = own.shape
    block = math.gcd(out_width, 512)
    count = len(offsets)

    def entry(at, k):
        return lax.rem(at[0] + k, line_count)

    in_specs = []
    operands = []
    own_shares, other_shares = by_shares(own_columns, share), other_columns
    for k in offsets:
        in_specs.append(column_spec(rows, share, lambda i, at, k=k: 2 * entry(at, k) + at[1]))
        in_specs.append(column_spec(rows, share, lambda i, at, k=k: entry(at, k)))
        operands += [own_shares, other_shares]
    in_specs += [pl.BlockSpec((rows, block), lambda i, at: (0, i))] * 2
    return pl.pallas_call(
        functools.partial(product_kernel, count),
        out_shape=[jax.ShapeDtypeStruct((share, out_width), BF16)] * count,
        grid_spec=pltpu.PrefetchScalarGridSpec(
            num_scalar_prefetch=1,
            grid=(out_width // block,),
            in_specs=in_specs,
            out_specs=[pl.BlockSpec((share, block), lambda i, at: (0, i))] * count,
            scratch_shapes=[pltpu.VMEM((count, share, 2 * rows), BF16)],
        ),
        cost_estimate=pl.CostEstimate(
            flops=4 * count * share * rows * out_width,
            bytes_accessed=4 * rows * out_width + 2 * count * share * (2 * rows + out_width),
            transcendentals=0,
        ),
        name="product",
    )(at, *operands, own, other)


def gate_kernel(normed_ref, gate_w_ref, up_w_ref, grad_act_ref, act_ref, grad_gate_ref, grad_up_ref):
    normed = normed_ref[...]
    gate = jnp.dot(normed, gate_w_ref[...], preferred_element_type=F32)
    upper = jnp.dot(normed, up_w_ref[...], preferred_element_type=F32)
    grad_act = grad_act_ref[...]
    sigma = jax.nn.sigmoid(gate)
    silu = gate * sigma
    act_ref[...] = (silu * upper).astype(BF16)
    grad_gate_ref[...] = (grad_act * upper * sigma * (1.0 + gate * (1.0 - sigma))).astype(BF16)
    grad_up_ref[...] = (grad_act * silu).astype(BF16)


def gate_and_up(normed, w_gate, w_up, grad_act):
    rows, width = normed.shape
    units = w_gate.shape[1]
    block = math.gcd(units, 256)
    wide = pl.BlockSpec((width, block), lambda i: (0, i))
    tall = pl.BlockSpec((rows, block), lambda i: (0, i))
    return pl.pallas_call(
        gate_kernel,
        out_shape=[jax.ShapeDtypeStruct((rows, units), BF16)] * 3,
        grid=(units // block,),
        in_specs=[pl.BlockSpec((rows, width), lambda i: (0, 0)), wide, wide, tall],
        out_specs=[tall] * 3,
        cost_estimate=pl.CostEstimate(
            flops=4 * rows * width * units,
            bytes_accessed=4 * width * units + 10 * rows * units,
            transcendentals=rows * units,
        ),
        name="gate_and_up",
    )(normed, w_gate, w_up, grad_act)


def norm_factor(values):
    return lax.rsqrt(jnp.mean(values * values, axis=-1, keepdims=True) + EPS)


def put_picked(picked, at_ref, in_ref, share, line_count):
    for pick_ref in picked:
        for i in range(line_count):
            column = pl.multiple_of((2 * i + 1 - at_ref[1]) * share, share)
            pick_ref[:, i * share : (i + 1) * share] = in_ref[:, pl.ds(column, share)]


def tile_of(half_ref, other_ref):
    return jnp.where(pl.program_id(0) < pl.num_programs(0) // 2, half_ref[...], other_ref[...]).astype(F32)


def entry_kernel(share, line_count, at_ref, x_ref, cot_ref, gain_ref, x_out, normed_out, cot_out, *picked):
    x = x_ref[0].astype(F32)
    x_out[...] = x_ref[0]
    cot_out[...] = cot_ref[0]
    normed_out[...] = (x * norm_factor(x) * gain_ref[...].astype(F32)).astype(BF16)
    put_picked(picked[:1], at_ref, normed_out, share, line_count)
    put_picked(picked[1:], at_ref, cot_out, share, line_count)


def norm2_kernel(share, line_count, at_ref, x_ref, att_half, att_other, gain_ref, normed_out, *picked):
    hidden = x_ref[...].astype(F32) + tile_of(att_half, att_other)
    normed_out[...] = (hidden * norm_factor(hidden) * gain_ref[...].astype(F32)).astype(BF16)
    put_picked(picked, at_ref, normed_out, share, line_count)


def norm_gradient(values, grad, gain, gain_out):
    factor = norm_factor(values)
    unit = values * factor

    @pl.when(pl.program_id(0) == 0)
    def _():
        gain_out[...] = jnp.zeros_like(gain_out)

    gain_out[...] += jnp.sum(grad * unit, axis=0, keepdims=True)
    scaled = grad * gain
    return factor * (scaled - unit * jnp.mean(scaled * unit, axis=-1, keepdims=True))


def back2_kernel(
    share, line_count, at_ref, x_ref, att_half, att_other, g_half, g_other, cot_ref, gain_ref, wide_out, out, gain_out, *picked
):
    hidden = x_ref[...].astype(F32) + tile_of(att_half, att_other)
    grad = norm_gradient(hidden, tile_of(g_half, g_other), gain_ref[...].astype(F32), gain_out)
    grad = grad + cot_ref[...].astype(F32)
    wide_out[...] = grad
    out[...] = grad.astype(BF16)
    put_picked(picked, at_ref, out, share, line_count)


def exit_kernel(
    at_ref, x_ref, att_half, att_other, f_half, f_other, g_half, g_other, wide_ref, gain_ref, block_out, grad_out, gain_out
):
    x = x_ref[...].astype(F32)
    block_out[0] = (x + tile_of(att_half, att_other) + tile_of(f_half, f_other)).astype(BF16)
    grad = norm_gradient(x, tile_of(g_half, g_other), gain_ref[...].astype(F32), gain_out)
    grad_out[0] = wide_ref[...] + grad


class Rows:
    def __init__(self, at, seqs, rows, width, share, line_count):
        self.at, self.seqs, self.rows, self.width = at, seqs, rows, width
        self.share, self.line_count = share, line_count
        self.tile = rows // 2
        self.count = seqs * 2
        self.whole_lanes = share % 128 == 0

    def outside(self):
        def index(i, at):
            seq = i // 2
            return (seq + at[2] - 2 * seq * at[2], lax.rem(i, 2), 0)

        return pl.BlockSpec((1, self.tile, self.width), index)

    def row(self, width=None):
        return pl.BlockSpec((self.tile, width or self.width), lambda i, at: (i, 0))

    def halves(self):
        half = self.count // 2
        shape = (self.tile, self.width)
        return [
            pl.BlockSpec(shape, lambda i, at: (jnp.minimum(i, half - 1), 0)),
            pl.BlockSpec(shape, lambda i, at: (jnp.maximum(i - half, 0), 0)),
        ]

    def line(self):
        return pl.BlockSpec((1, self.width), lambda i, at: (0, 0))

    def array(self, dtype, width=None):
        return jax.ShapeDtypeStruct((self.count * self.tile, width or self.width), dtype)

    def call(self, name, kernel, in_specs, operands, out_specs, outs, picks=0):
        if self.whole_lanes and picks:
            kept = self.share * self.line_count
            out_specs = out_specs + [self.row(kept)] * picks
            outs = outs + [self.array(BF16, kept)] * picks
        moved = sum(math.prod(o.shape) * o.dtype.itemsize for o in list(outs) + list(operands))
        return pl.pallas_call(
            kernel,
            out_shape=outs,
            grid_spec=pltpu.PrefetchScalarGridSpec(
                num_scalar_prefetch=1, grid=(self.count,), in_specs=in_specs, out_specs=out_specs
            ),
            cost_estimate=pl.CostEstimate(flops=0, bytes_accessed=moved, transcendentals=0),
            name=name,
        )(self.at, *operands)

    def picked(self, array, rest):
        if self.whole_lanes:
            return rest
        return pick_columns(self.at, array, self.share, self.line_count)

    def entry(self, x, cot, gain):
        x, normed, cot, *rest = self.call(
            "entry",
            functools.partial(entry_kernel, self.share, self.line_count),
            [self.outside(), self.outside(), self.line()],
            [x, cot, gain],
            [self.row()] * 3,
            [self.array(BF16)] * 3,
            picks=2,
        )
        rest = rest or [None, None]
        return x, normed, cot, self.picked(normed, rest[0]), self.picked(cot, rest[1])

    def norm2(self, x, att, gain):
        normed, *rest = self.call(
            "norm2",
            functools.partial(norm2_kernel, self.share, self.line_count),
            [self.row()] + self.halves() + [self.line()],
            [x, *att, gain],
            [self.row()],
            [self.array(BF16)],
            picks=1,
        )
        return normed, self.picked(normed, rest[0] if rest else None)

    def back2(self, x, att, grad, cot, gain):
        wide, narrow, gain_grad, *rest = self.call(
            "back2",
            functools.partial(back2_kernel, self.share, self.line_count),
            [self.row()] + self.halves() * 2 + [self.row(), self.line()],
            [x, *att, *grad, cot, gain],
            [self.row(), self.row(), self.line()],
            [self.array(F32), self.array(BF16), jax.ShapeDtypeStruct((1, self.width), F32)],
            picks=1,
        )
        return wide, narrow, gain_grad, self.picked(narrow, rest[0] if rest else None)

    def exit(self, x, att, ffn, grad, wide, gain):
        shape = (self.seqs, self.rows, self.width)
        return self.call(
            "exit",
            exit_kernel,
            [self.row()] + self.halves() * 3 + [self.row(), self.line()],
            [x, *att, *ffn, *grad, wide, gain],
            [self.outside(), self.outside(), self.line()],
            [
                jax.ShapeDtypeStruct(shape, BF16),
                jax.ShapeDtypeStruct(shape, F32),
                jax.ShapeDtypeStruct((1, self.width), F32),
            ],
        )


def sum_bf16(*terms):
    total = terms[0].astype(F32)
    for term in terms[1:]:
        total = total + term.astype(F32)
    return total.astype(BF16)


def swap(array, axis, bit, count):
    return lax.ppermute(array, axis, [(i, i ^ bit) for i in range(count)])


def sum_over_tp(part, tp_count):
    rows = part.shape[0] // 2
    half = sum_bf16(part[:rows], swap(part[rows:], "tp", 1, tp_count))
    bit = 2
    while bit < tp_count:
        half = sum_bf16(half, swap(half, "tp", bit, tp_count))
        bit *= 2
    return half, swap(half, "tp", 1, tp_count)


def line_scatter(parts, line_count):
    up = down = None
    last = line_count - 1
    for step in range(1, line_count):
        send_up, send_down = parts[line_count - step], parts[step]
        if up is not None:
            send_up = sum_bf16(send_up, up)
            send_down = sum_bf16(send_down, down)
        up = lax.ppermute(
            send_up, "ctx", [(2 * i + x, 2 * i + 2 + x) for i in range(step) for x in range(2)]
        )
        down = lax.ppermute(
            send_down,
            "ctx",
            [(2 * (last - i) + x, 2 * (last - i) - 2 + x) for i in range(step) for x in range(2)],
        )
    total = parts[0].astype(F32)
    if up is not None:
        total = total + up.astype(F32) + down.astype(F32)
    return total


def after(value, *others):
    return lax.optimization_barrier((value,) + others)[0]


def rope_table(positions):
    freq = jnp.exp(jnp.arange(HALF, dtype=F32) * (-2.0 * math.log(ROPE_BASE) / HEAD_DIM))
    angle = positions.astype(F32)[:, None, :] * freq[None, :, None]
    return jnp.cos(angle)[:, None], jnp.sin(angle)[:, None]


def rotate_t(values, cosine, sine):
    halves, width, keys = values.shape
    split = values.reshape(halves, width // HEAD_DIM, 2, HALF, keys)
    first, second = split[:, :, 0], split[:, :, 1]
    return jnp.stack(
        [first * cosine - second * sine, second * cosine + first * sine], axis=2
    ).reshape(values.shape)


def on_device(
    ctx_count,
    tp_count,
    layer_input,
    attn_gain,
    w_query,
    w_key,
    w_value,
    w_out,
    ffn_gain,
    w_gate,
    w_up,
    w_down,
    cotangent,
    block_ids,
    doc_ids,
):
    seqs, rows, width = layer_input.shape
    block_len = rows // 2
    halves = seqs * 2
    block_total = block_ids.shape[1]
    q_width, kv_width = w_query.shape[1], w_key.shape[1]
    kv_heads = kv_width // HEAD_DIM
    group = q_width // kv_width
    tokens = seqs * rows
    share = width // ctx_count
    place = lax.axis_index("ctx")
    line_count = ctx_count // 2
    line, side = place // 2, place % 2
    core = lax.axis_index("tp") % 2
    at = jnp.stack([line, side, core]).astype(jnp.int32)
    tiles = Rows(at, seqs, rows, width, share, line_count)

    def own_first(array):
        return jnp.where(core == 0, array, array[::-1])

    def pair(array):
        return swap(array, "ctx", 1, ctx_count)

    def weight_grad(columns, grads, other_grads):
        parts = [None] * line_count
        for step in range(1, line_count // 2 + 1):
            offsets = sorted({line_count - step, step})
            if step == line_count // 2:
                offsets = offsets + [0]
            outs = product(at, *columns, grads, other_grads, offsets, share, line_count)
            for k, out in zip(offsets, outs):
                parts[k] = out
        return line_scatter(parts, line_count)

    block_ids = own_first(block_ids)
    doc_ids = own_first(doc_ids)

    slot_index = jnp.arange(block_total, dtype=jnp.int32)
    slots = jnp.sum(
        jnp.where(block_ids[:, :, None] == slot_index[None, None, :], slot_index[None, :, None], 0),
        axis=1,
    )
    own_blocks = lax.dynamic_slice_in_dim(block_ids, 2 * place, 2, 1).reshape(halves)
    positions = own_blocks[:, None] * block_len + jnp.arange(block_len, dtype=jnp.int32)[None, :]
    docs = jnp.concatenate(
        [
            lax.dynamic_slice(doc_ids, (i // 2, own_blocks[i] * block_len), (1, block_len))
            for i in range(halves)
        ],
        axis=1,
    ).reshape(seqs, rows)
    first_key = jnp.sum((doc_ids[:, :, None] < docs[:, None, :]).astype(jnp.int32), axis=1).reshape(
        halves, block_len
    )
    bounds = jnp.stack([first_key, positions], axis=1)
    low_blocks = first_key[:, 0] // block_len
    cosine, sine = rope_table(positions)

    attn_gain, ffn_gain = attn_gain.reshape(1, width), ffn_gain.reshape(1, width)
    x, normed1, cot, n1_pick, cot_pick = tiles.entry(layer_input, cotangent, attn_gain)
    tiles1 = normed1.reshape(halves, block_len, width)

    def project_t(weight):
        return jnp.einsum("dc,htd->hct", weight, tiles1, preferred_element_type=F32)

    key_t = rotate_t(project_t(w_key), cosine, sine).astype(BF16)
    value_t = project_t(w_value).astype(BF16)
    kv_own = jnp.concatenate([key_t, value_t], axis=1)
    kv_all = lax.all_gather(kv_own, "ctx", axis=0, tiled=True)
    scale = HEAD_DIM ** (-0.5)
    query_t = (rotate_t(project_t(w_query), cosine, sine)).astype(BF16) * jnp.asarray(scale, BF16)
    n1_other, cot_other = pair(n1_pick), pair(cot_pick)
    grad_act = jnp.einsum("td,fd->tf", cot, w_down, preferred_element_type=F32)
    query_t = after(query_t, grad_act)
    att_t, lse = attend_forward(
        slots, own_blocks, low_blocks, query_t, kv_all, bounds, kv_heads, group
    )
    attended = jnp.transpose(att_t, (0, 2, 1)).reshape(tokens, q_width)
    attn_part = jnp.dot(attended, w_out, preferred_element_type=F32).astype(BF16)
    att_sum = sum_over_tp(attn_part, tp_count)

    normed2, n2_pick = tiles.norm2(x, att_sum, ffn_gain)
    act, grad_gate, grad_upper = gate_and_up(normed2, w_gate, w_up, grad_act)
    other_act = pair(after(act, cot_other, n1_other))
    grad_n2_part = (
        jnp.einsum("tf,df->td", grad_gate, w_gate, preferred_element_type=F32)
        + jnp.einsum("tf,df->td", grad_upper, w_up, preferred_element_type=F32)
    ).astype(BF16)
    grad_n2 = sum_over_tp(grad_n2_part, tp_count)
    ffn_part = jnp.dot(after(act, grad_n2_part), w_down, preferred_element_type=F32).astype(BF16)
    ffn_sum = sum_over_tp(ffn_part, tp_count)
    n2_other = pair(after(n2_pick, other_act))
    other_gate = pair(after(grad_gate, n2_other))
    other_upper = pair(after(grad_upper, other_gate))
    grad_w_down = weight_grad((cot, cot_other), after(act, ffn_part), other_act)
    grad_hidden, grad_hidden_b, grad_ffn_gain, gh_pick = tiles.back2(x, att_sum, grad_n2, cot, ffn_gain)

    do_t = jnp.einsum(
        "cd,htd->hct",
        w_out,
        grad_hidden_b.reshape(halves, block_len, width),
        preferred_element_type=F32,
    ).astype(BF16)
    dq_t, dkv_part = attend_backward(
        slots, own_blocks, low_blocks, query_t, kv_all, bounds, att_t, lse, do_t, kv_heads, group
    )
    grad_w_gate = weight_grad((normed2, n2_other), after(grad_gate, dq_t), other_gate)
    grad_w_up = weight_grad((normed2, n2_other), after(grad_upper, dq_t), other_upper)
    gh_other = pair(after(gh_pick, other_upper))
    att_other = pair(after(attended, other_upper))
    grad_w_out = weight_grad((grad_hidden_b, gh_other), attended, att_other)
    dkv_split = dkv_part.reshape((line_count, 2) + kv_own.shape)
    dkv_mine = lax.dynamic_index_in_dim(dkv_split, side, 1, keepdims=False)
    dkv_theirs = lax.dynamic_index_in_dim(dkv_split, 1 - side, 1, keepdims=False)
    dkv_pair = sum_bf16(dkv_mine, pair(dkv_theirs))
    dkv = line_scatter(
        [
            lax.dynamic_index_in_dim(dkv_pair, lax.rem(line + k, line_count), 0, keepdims=False)
            for k in range(line_count)
        ],
        line_count,
    )
    grad_query_t = (rotate_t(dq_t, cosine, -sine) * scale).astype(BF16)
    grad_key_t = rotate_t(dkv[:, :kv_width], cosine, -sine).astype(BF16)
    grad_value_t = dkv[:, kv_width:].astype(BF16)
    grad_qkv = jnp.transpose(
        jnp.concatenate([grad_query_t, grad_key_t, grad_value_t], axis=1), (0, 2, 1)
    ).reshape(tokens, q_width + 2 * kv_width)
    w_qkv = jnp.concatenate([w_query, w_key, w_value], axis=1)
    grad_n1_part = jnp.einsum(
        "tc,dc->td", grad_qkv, w_qkv, preferred_element_type=F32
    ).astype(BF16)
    grad_n1 = sum_over_tp(grad_n1_part, tp_count)
    qkv_other = pair(after(grad_qkv, other_upper))
    grad_w_qkv = weight_grad((normed1, n1_other), grad_qkv, qkv_other)
    block_out, grad_input, grad_attn_gain = tiles.exit(x, att_sum, ffn_sum, grad_n1, grad_hidden, attn_gain)
    gains = jnp.concatenate([grad_attn_gain, grad_ffn_gain]).reshape(2, ctx_count, share)
    gains = jnp.sum(lax.all_to_all(gains, "ctx", 1, 1, tiled=True), axis=1)
    return (
        block_out,
        grad_input,
        gains[0],
        grad_w_qkv[:, :q_width],
        grad_w_qkv[:, q_width : q_width + kv_width],
        grad_w_qkv[:, q_width + kv_width :],
        grad_w_out.T,
        gains[1],
        grad_w_gate,
        grad_w_up,
        grad_w_down.T,
    )


def solution(mesh):
    in_specs = (
        P(None, "ctx", None),
        P(),
        P(None, "tp"),
        P(None, "tp"),
        P(None, "tp"),
        P("tp", None),
        P(),
        P(None, "tp"),
        P(None, "tp"),
        P("tp", None),
        P(None, "ctx", None),
        P(),
        P(),
    )
    out_specs = (
        P(None, "ctx", None),
        P(None, "ctx", None),
        P("ctx"),
        P("ctx", "tp"),
        P("ctx", "tp"),
        P("ctx", "tp"),
        P("tp", "ctx"),
        P("ctx"),
        P("ctx", "tp"),
        P("ctx", "tp"),
        P("tp", "ctx"),
    )
    return jax.shard_map(
        functools.partial(on_device, mesh.shape["ctx"], mesh.shape["tp"]),
        mesh=mesh,
        in_specs=in_specs,
        out_specs=out_specs,
        check_vma=False,
    )
```
